32 devices in a mesh: kx: 2 (over x), ky: 4 (over y, core), kz: 4 (over z).
Axes of the slice: x: 2, y: 2, z: 4, core: 2. Of those that a mesh axis runs over, the one named last changes fastest.
Arguments:
- coefficients: bfloat16 [2, 2, 4, 4, 512, 2048], P(None, 'kx', 'ky', 'kz'), may hold values from -1 to 1
- shift_blocks: int32 [3], replicated, may hold values from 1 to 15, as said below
Outputs:
- centre: float32 [3, 512], replicated
- spread: float32 [3, 512], replicated
- coherence: float32 [3, 2, 4, 4], P(None, 'kx', 'ky', 'kz')
The draws below stay inside these ranges and needn't reach their ends.
Inputs may be any that keep to these rules, and one draw needn't show every extreme that they name: The coefficients one period further along direction d are those of the first k-point of the string with plane-wave index g read at (g + 128 * shift_blocks[d]) mod 2048.
All inputs are finite; a program needn't handle non-finite values.
Results may differ from the reference program's by a relative error of at most 0.0003.
Values may be sent and summed in bfloat16 or wider, within the bound.
No kernel may reach another device: no remote copies, remote signals or barrier semaphores. Data moves between devices by JAX's collectives and lax.ppermute only.
A program may use at most 128 MiB of HBM per device.

```python
import jax
import jax.numpy as jnp
from jax import lax

NB = 512
NGW = 2048
NX = 2
NY = 4
NZ = 4


def offsets_for(key):
    middle = jax.random.randint(jax.random.fold_in(key, 11), (1,), 1, NGW // 128).astype(jnp.int32)
    ends = jnp.array([1, NGW // 128 - 1], jnp.int32)
    values = jnp.concatenate([ends, middle])
    order = jax.random.permutation(jax.random.fold_in(key, 13), 3)
    return values[order].astype(jnp.int32)


def draw_shift_blocks(key, part):
    return offsets_for(key)


def mix_along(fields, shift, points, position):
    angles = jnp.arange(points, dtype=jnp.float32) * (jnp.pi / (2.0 * points))
    dims_shape = [1] * (fields.ndim + 1)
    dims_shape[position] = points
    cosine = jnp.cos(angles).reshape(dims_shape)
    sine = jnp.sin(angles).reshape(dims_shape)
    rolled = jnp.roll(fields, -shift, axis=-1)
    return cosine * jnp.expand_dims(fields, position) + sine * jnp.expand_dims(rolled, position)


def draw_coefficients(key, part):
    offsets = offsets_for(key) * 128
    subkeys = jax.random.split(jax.random.fold_in(key, 23), 5)
    entry_scale = 1.0 / jnp.sqrt(2.0 * NGW)
    common = jnp.clip(jax.random.normal(subkeys[0], (2, NB, NGW), jnp.float32), -6.0, 6.0) * entry_scale
    fields = mix_along(common, offsets[2], NZ, 1)
    fields = mix_along(fields, offsets[1], NY, 1)
    fields = mix_along(fields, offsets[0], NX, 1)
    full_shape = (2, NX, NY, NZ, NB, NGW)
    roughness = jnp.clip(jax.random.normal(subkeys[1], full_shape, jnp.float32), -6.0, 6.0)
    amplitude = jnp.exp(jax.random.uniform(subkeys[2], (NB,), jnp.float32, jnp.log(0.1), jnp.log(0.6)))
    jitter = 0.35
    fields = fields + amplitude[:, None] * roughness * entry_scale
    winding = jax.random.uniform(subkeys[3], (3, NB), jnp.float32, -0.2, 0.2)
    x_frac = jnp.arange(NX, dtype=jnp.float32) / NX
    y_frac = jnp.arange(NY, dtype=jnp.float32) / NY
    z_frac = jnp.arange(NZ, dtype=jnp.float32) / NZ
    angles = 2.0 * jnp.pi * (winding[0] * x_frac[:, None, None, None] + winding[1] * y_frac[None, :, None, None] + winding[2] * z_frac[None, None, :, None])
    angles = angles + jax.random.uniform(subkeys[4], (NX, NY, NZ, NB), jnp.float32, -jitter, jitter)
    cosine = jnp.cos(angles)[..., None]
    sine = jnp.sin(angles)[..., None]
    real_part = cosine * fields[0] - sine * fields[1]
    imag_part = sine * fields[0] + cosine * fields[1]
    return jnp.stack([real_part, imag_part]).astype(jnp.bfloat16)


def setup_inputs(seed: int = 0) -> dict:
    arg_keys = jax.random.split(jax.random.key(seed), 3)
    coefficients = draw_coefficients(jax.random.fold_in(arg_keys[2], 71), 0)
    shift_blocks = draw_shift_blocks(jax.random.fold_in(arg_keys[2], 71), 0)
    return dict(coefficients=coefficients, shift_blocks=shift_blocks)


def pair_measure(own_point, partner):
    bands = own_point.shape[1]
    left_side = jnp.concatenate([own_point[0], own_point[1]], axis=1)
    right_side = jnp.concatenate([jnp.concatenate([partner[0], partner[1]], axis=1), jnp.concatenate([partner[1], -partner[0]], axis=1)], axis=0)
    product = jnp.dot(left_side, right_side.T, preferred_element_type=jnp.float32)
    real_part = product[:, :bands]
    imag_part = product[:, bands:]
    phases = jnp.arctan2(jnp.diagonal(imag_part), jnp.diagonal(real_part))
    coherence = jnp.sum(real_part * real_part + imag_part * imag_part) / bands
    return phases, coherence


def reference(coefficients, shift_blocks):
    shifts = shift_blocks.astype(jnp.int32) * 128
    k_total = NX * NY * NZ
    counts = jnp.array([NX, NY, NZ], jnp.float32)

    def per_point(k_index):
        x_index = k_index // (NY * NZ)
        y_index = (k_index // NZ) % NY
        z_index = k_index % NZ
        own_point = coefficients[:, x_index, y_index, z_index]
        gathered_phases = []
        gathered_coherence = []
        for direction in range(3):
            coords = [x_index, y_index, z_index]
            limits = [NX, NY, NZ]
            wrapped = coords[direction] == limits[direction] - 1
            coords[direction] = (coords[direction] + 1) % limits[direction]
            partner = coefficients[:, coords[0], coords[1], coords[2]]
            partner = jnp.where(wrapped, jnp.roll(partner, -shifts[direction], axis=-1), partner)
            phases, coherence = pair_measure(own_point, partner)
            gathered_phases.append(phases)
            gathered_coherence.append(coherence)
        return jnp.stack(gathered_phases), jnp.stack(gathered_coherence)

    phases, coherence = lax.map(per_point, jnp.arange(k_total, dtype=jnp.int32))
    mean_phase = jnp.sum(phases, axis=0) / k_total
    deviation = phases - mean_phase[None]
    variance = jnp.sum(deviation * deviation, axis=0) / k_total
    centre = -counts[:, None] * mean_phase / (2.0 * jnp.pi)
    spread = (counts[:, None] / (2.0 * jnp.pi)) ** 2 * variance
    coherence_out = coherence.T.reshape(3, NX, NY, NZ)
    return centre, spread, coherence_out
```

```python
import functools

import jax
import jax.numpy as jnp
from jax import lax
from jax.experimental import pallas as pl
from jax.experimental.pallas import tpu as pltpu
from jax.sharding import PartitionSpec as P

LANES = 128
AXES = ("kx", "ky", "kz")


def passed_along(value, axis, steps):
    count = lax.axis_size(axis)
    pairs = [(source, (source + steps) % count) for source in range(count)]
    return lax.ppermute(value, axis, pairs)


def exchanged(value, axis, mask):
    pairs = [(source, source ^ mask) for source in range(lax.axis_size(axis))]
    return lax.ppermute(value, axis, pairs)


def reduced(value):
    for axis in ("ky", "kx", "kz"):
        count = lax.axis_size(axis)
        if count & (count - 1):
            value = lax.psum(value, axis)
            continue
        mask = 1
        while mask < count:
            value = value + exchanged(value, axis, mask)
            mask *= 2
    return value


def chunk_kernel(start, directions, shift_ref, own_ref, *refs):
    count = len(directions)
    chunk_refs = refs[:count]
    out_ref, rolled = refs[count], refs[count + 1]
    bands = own_ref.shape[0] // 2
    rows = rolled.shape[0]
    width = rolled.shape[1]
    blocks = width // LANES
    size = rows // 2
    for slot, direction in enumerate(directions):
        chunk_ref = chunk_refs[slot]
        shift = shift_ref[direction]
        for block in range(blocks):
            source = lax.rem(shift + block, blocks) * LANES
            rolled[:, block * LANES : (block + 1) * LANES] = chunk_ref[
                :, pl.ds(pl.multiple_of(source, LANES), LANES)
            ]
        product = lax.dot_general(
            own_ref[...], rolled[...], (((1,), (1,)), ((), ())), preferred_element_type=jnp.float32
        )
        real_part = product[:bands, :size] + product[bands:, size:]
        imag_part = product[:bands, size:] - product[bands:, :size]
        squares = jnp.sum(real_part * real_part + imag_part * imag_part, axis=0, keepdims=True)
        row = lax.broadcasted_iota(jnp.int32, (size, size), 0)
        column = lax.broadcasted_iota(jnp.int32, (size, size), 1)
        on_diagonal = row == column
        real_diag = jnp.sum(
            jnp.where(on_diagonal, real_part[start : start + size], 0.0), axis=0, keepdims=True
        )
        imag_diag = jnp.sum(
            jnp.where(on_diagonal, imag_part[start : start + size], 0.0), axis=0, keepdims=True
        )
        out_ref[slot, 0:1, :] = jnp.arctan2(imag_diag, real_diag)
        out_ref[slot, 1:2, :] = squares


def chunk_measure(shift, own, chunks, start, directions):
    rows, width = chunks[0].shape
    return pl.pallas_call(
        functools.partial(chunk_kernel, start, directions),
        out_shape=jax.ShapeDtypeStruct((len(chunks), 2, rows // 2), jnp.float32),
        in_specs=[pl.BlockSpec(memory_space=pltpu.SMEM)]
        + [pl.BlockSpec(memory_space=pltpu.VMEM)] * (1 + len(chunks)),
        out_specs=pl.BlockSpec(memory_space=pltpu.VMEM),
        scratch_shapes=[pltpu.VMEM((rows, width), chunks[0].dtype)],
        compiler_params=pltpu.CompilerParams(vmem_limit_bytes=32 * 1024 * 1024),
        name=f"pairs_{start}_" + "".join(str(d) for d in directions),
    )(shift, own, *chunks)


def shards(coefficients, shift_blocks):
    bands, width = coefficients.shape[4:]
    point = coefficients.reshape(2, bands, width)
    own = coefficients.reshape(2 * bands, width)
    wraps = jnp.stack([lax.axis_index(a) == lax.axis_size(a) - 1 for a in AXES])
    shift = jnp.where(wraps, shift_blocks, 0)
    quarter = bands // 4
    y_later = passed_along(point, "ky", -1).reshape(2 * bands, width)
    received = []
    for start in range(0, bands, quarter):
        piece = point[:, start : start + quarter]
        z_piece = passed_along(piece, "kz", -1).reshape(2 * quarter, width)
        x_piece = passed_along(piece, "kx", -1).reshape(2 * quarter, width)
        received.append((x_piece, z_piece))
    y_out = chunk_measure(shift, own, [y_later], 0, (1,))
    parts = [
        chunk_measure(shift, own, list(pieces), index * quarter, (0, 2))
        for index, pieces in enumerate(received)
    ]
    xz_out = jnp.concatenate(parts, axis=2)
    table = jnp.stack([xz_out[0], y_out[0], xz_out[1]])
    phases = table[:, 0]
    coherence = (jnp.sum(table[:, 1], axis=1) / bands).reshape(3, 1, 1, 1)
    k_total = 1
    for a in AXES:
        k_total *= lax.axis_size(a)
    counts = jnp.array([[lax.axis_size(a)] for a in AXES], jnp.float32)
    sums = reduced(jnp.concatenate([phases, phases * phases]))
    mean_phase = sums[:3] / k_total
    variance = sums[3:] / k_total - mean_phase * mean_phase
    centre = -counts * mean_phase / (2.0 * jnp.pi)
    spread = (counts / (2.0 * jnp.pi)) ** 2 * variance
    return (centre, spread, coherence)


def solution(mesh):
    in_specs = (P(None, "kx", "ky", "kz", None, None), P())
    out_specs = (P(), P(), P(None, "kx", "ky", "kz"))
    return jax.shard_map(shards, mesh=mesh, in_specs=in_specs, out_specs=out_specs, check_vma=False)
```

```python
import functools

import jax
import jax.numpy as jnp
from jax import lax
from jax.experimental import pallas as pl
from jax.experimental.pallas import tpu as pltpu
from jax.sharding import PartitionSpec as P

LANES = 128
AXES = ("kx", "ky", "kz")


def takes_x(x, y):
    return (x + y) % 2 == 0


def fetched(value, source_of):
    nx, ny, nz = (lax.axis_size(a) for a in AXES)
    pairs = []
    for x in range(nx):
        for y in range(ny):
            for z in range(nz):
                source = source_of(x, y, z)
                if source is not None:
                    sx, sy, sz = source[0] % nx, source[1] % ny, source[2] % nz
                    pairs.append(((sx * ny + sy) * nz + sz, (x * ny + y) * nz + z))
    return lax.ppermute(value, AXES, pairs)


def passed_along(value, axis, steps):
    count = lax.axis_size(axis)
    pairs = [(source, (source + steps) % count) for source in range(count)]
    return lax.ppermute(value, axis, pairs)


def exchanged(value, axis, mask):
    pairs = [(source, source ^ mask) for source in range(lax.axis_size(axis))]
    return lax.ppermute(value, axis, pairs)


def reduced(value):
    for axis in ("ky", "kx", "kz"):
        count = lax.axis_size(axis)
        if count & (count - 1):
            value = lax.psum(value, axis)
            continue
        mask = 1
        while mask < count:
            value = value + exchanged(value, axis, mask)
            mask *= 2
    return value


def roll_into(rolled, source_ref, shift):
    blocks = rolled.shape[1] // LANES
    for block in range(blocks):
        source = lax.rem(shift + block, blocks) * LANES
        rolled[:, block * LANES : (block + 1) * LANES] = source_ref[
            :, pl.ds(pl.multiple_of(source, LANES), LANES)
        ]


def pair_rows(own_ref, rolled, start, reverse):
    bands = own_ref.shape[0] // 2
    size = rolled.shape[0] // 2
    product = lax.dot_general(
        own_ref[...], rolled[...], (((1,), (1,)), ((), ())), preferred_element_type=jnp.float32
    )
    real_part = product[:bands, :size] + product[bands:, size:]
    imag_part = product[:bands, size:] - product[bands:, :size]
    squares = jnp.sum(real_part * real_part + imag_part * imag_part, axis=0, keepdims=True)
    row = lax.broadcasted_iota(jnp.int32, (size, size), 0)
    column = lax.broadcasted_iota(jnp.int32, (size, size), 1)
    near = row == column
    real_diag = jnp.sum(jnp.where(near, real_part[start : start + size], 0.0), axis=0, keepdims=True)
    imag_diag = jnp.sum(jnp.where(near, imag_part[start : start + size], 0.0), axis=0, keepdims=True)
    if reverse:
        imag_diag = jnp.where(imag_diag == 0.0, 0.0, -imag_diag)
    return jnp.arctan2(imag_diag, real_diag), squares


def plane_kernel(scalars, own_ref, ahead_ref, behind_ref, token_ref, out_ref, rolled):
    roll_into(rolled, ahead_ref, scalars[0])
    phases, squares = pair_rows(own_ref, rolled, 0, False)
    out_ref[0:1, :] = phases
    out_ref[2:3, :] = squares

    @pl.when(scalars[4] == 1)
    def _():
        roll_into(rolled, ahead_ref, scalars[1])

    @pl.when(scalars[4] == 0)
    def _():
        roll_into(rolled, behind_ref, scalars[1])

    phases, squares = pair_rows(own_ref, rolled, 0, True)
    out_ref[1:2, :] = phases
    out_ref[3:4, :] = squares


def string_kernel(start, scalars, own_ref, chunk_ref, *refs):
    out_ref, rolled = refs[-2], refs[-1]
    roll_into(rolled, chunk_ref, scalars[2])
    phases, squares = pair_rows(own_ref, rolled, start, False)
    out_ref[0:1, :] = phases
    out_ref[1:2, :] = squares


def last_kernel(starts, scalars, own_ref, chunk_ref, plane_ref, *refs):
    earlier, sums_ref, squares_ref, rolled = refs[:-3], refs[-3], refs[-2], refs[-1]
    roll_into(rolled, chunk_ref, scalars[2])
    phases, squares = pair_rows(own_ref, rolled, starts[-1], False)
    ahead, behind = plane_ref[0:1, :], plane_ref[1:2, :]
    total = ahead + behind
    total_squares = ahead * ahead + behind * behind
    along_x = scalars[3] == 1
    zero = jnp.zeros_like(total)
    sums_ref[0:1, :] = jnp.where(along_x, total, zero)
    sums_ref[1:2, :] = jnp.where(along_x, zero, total)
    sums_ref[3:4, :] = jnp.where(along_x, total_squares, zero)
    sums_ref[4:5, :] = jnp.where(along_x, zero, total_squares)
    sums_ref[6:7, :] = zero
    sums_ref[7:8, :] = zero
    for start, ref in zip(starts, earlier):
        stop = start + ref.shape[1]
        sums_ref[2:3, start:stop] = ref[0:1, :]
        sums_ref[5:6, start:stop] = ref[0:1, :] * ref[0:1, :]
        squares_ref[0:1, start:stop] = ref[1:2, :]
    stop = starts[-1] + phases.shape[1]
    sums_ref[2:3, starts[-1] : stop] = phases
    sums_ref[5:6, starts[-1] : stop] = phases * phases
    squares_ref[0:1, starts[-1] : stop] = squares


def on_core(kernel, scalars, operands, outs, scratch_shape, name, grant):
    return pl.pallas_call(
        kernel,
        out_shape=outs,
        in_specs=[pl.BlockSpec(memory_space=pltpu.SMEM)]
        + [pl.BlockSpec(memory_space=pltpu.VMEM)] * len(operands),
        out_specs=jax.tree.map(lambda _: pl.BlockSpec(memory_space=pltpu.VMEM), outs),
        scratch_shapes=[pltpu.VMEM(scratch_shape, operands[0].dtype)],
        compiler_params=pltpu.CompilerParams(vmem_limit_bytes=grant * 1024 * 1024),
        name=name,
    )(scalars, *operands)


def shards(coefficients, shift_blocks):
    bands, width = coefficients.shape[4:]
    nx, ny, nz = (lax.axis_size(a) for a in AXES)
    if coefficients.shape[1:4] != (1, 1, 1) or nx % 2 or ny % 2:
        raise ValueError("unsupported mesh")
    x, y, z = (lax.axis_index(a) for a in AXES)
    point = coefficients.reshape(2, bands, width)
    own = coefficients.reshape(2 * bands, width)
    blocks = width // LANES
    quarter = bands // 4
    sizes = (quarter, bands - 2 * quarter, quarter)
    starts = (0, quarter, bands - quarter)

    pieces = [point[:, : sizes[0]]]
    rest = lax.optimization_barrier((point, pieces[0]))[0]
    pieces += [rest[:, s : s + n] for s, n in zip(starts[1:], sizes[1:])]
    z_pieces = [passed_along(pieces[0], "kz", -1)]
    ahead = fetched(point, lambda i, j, k: (i + 1, j, k) if takes_x(i, j) else (i, j + 1, k))

    def behind_of(i, j, k):
        if takes_x(i, j):
            return None if nx == 2 else (i - 1, j, k)
        return (i, j - 1, k)

    behind = fetched(point, behind_of)
    z_pieces += [passed_along(p, "kz", -1) for p in pieces[1:]]
    ahead, behind = ahead.reshape(2 * bands, width), behind.reshape(2 * bands, width)
    z_pieces = [p.reshape(2 * n, width) for p, n in zip(z_pieces, sizes)]

    along_x = takes_x(x, y)
    place = jnp.where(along_x, x, y)
    last = jnp.where(along_x, nx, ny) - 1
    plane_shift = jnp.where(along_x, shift_blocks[0], shift_blocks[1])
    scalars = jnp.stack(
        [
            jnp.where(place == last, plane_shift, 0),
            jnp.where(place == 0, blocks - plane_shift, 0),
            jnp.where(z == nz - 1, shift_blocks[2], 0),
            along_x.astype(jnp.int32),
            (along_x & (nx == 2)).astype(jnp.int32),
        ]
    ).astype(jnp.int32)

    def row_out(n):
        return jax.ShapeDtypeStruct((2, n), jnp.float32)

    first = on_core(
        functools.partial(string_kernel, starts[0]), scalars, [own, z_pieces[0]],
        row_out(sizes[0]), (2 * sizes[0], width), "string_first", 20,
    )
    plane = on_core(
        plane_kernel, scalars, [own, ahead, behind, first],
        jax.ShapeDtypeStruct((4, bands), jnp.float32), (2 * bands, width), "plane", 44,
    )
    plane_coherence = jnp.sum(plane[2:], axis=1) / bands
    passed_on = fetched(
        plane_coherence[1:], lambda i, j, k: (i, j + 1, k) if takes_x(i, j) else (i + 1, j, k)
    )
    middle = on_core(
        functools.partial(string_kernel, starts[1]), scalars, [own, z_pieces[1], plane],
        row_out(sizes[1]), (2 * sizes[1], width), "string_middle", 24,
    )
    middle, passed_on = lax.optimization_barrier((middle, passed_on))
    sums, squares = on_core(
        functools.partial(last_kernel, starts), scalars, [own, z_pieces[2], plane, first, middle],
        [jax.ShapeDtypeStruct((8, bands), jnp.float32), jax.ShapeDtypeStruct((1, bands), jnp.float32)],
        (2 * sizes[2], width), "string_last", 20,
    )
    z_coherence = jnp.sum(squares) / bands
    kept, given = plane_coherence[0], passed_on[0]
    coherence = jnp.stack(
        [jnp.where(along_x, kept, given), jnp.where(along_x, given, kept), z_coherence]
    ).reshape(3, 1, 1, 1)
    k_total = nx * ny * nz
    counts = jnp.array([[nx], [ny], [nz]], jnp.float32)
    sums = reduced(sums)
    mean_phase = sums[:3] / k_total
    variance = sums[3:6] / k_total - mean_phase * mean_phase
    centre = -counts * mean_phase / (2.0 * jnp.pi)
    spread = (counts / (2.0 * jnp.pi)) ** 2 * variance
    return (centre, spread, coherence)


def solution(mesh):
    in_specs = (P(None, "kx", "ky", "kz", None, None), P())
    out_specs = (P(), P(), P(None, "kx", "ky", "kz"))
    return jax.shard_map(shards, mesh=mesh, in_specs=in_specs, out_specs=out_specs, check_vma=False)
```
